8 devices in a mesh: depth: 2 (over z, y), col: 2 (over x), row: 2 (over core).
Axes of the slice: x: 2, y: 2, z: 1, core: 2. Of those that a mesh axis runs over, the one named last changes fastest.
Arguments:
- tokens: bfloat16 [4096, 4096], P(('depth', 'row'), 'col')
- w_up: bfloat16 [4096, 11008], P('row', 'col')
- w_down: bfloat16 [11008, 4096], P('row', 'col')
- w_value: bfloat16 [4096, 4096], P('row', 'col')
- w_output: bfloat16 [4096, 4096], P('row', 'col')
- grad_out: bfloat16 [4096, 4096], P(('depth', 'row'), 'col')
Outputs:
- output 1: bfloat16 [4096, 4096], P(('depth', 'row'), 'col')
- output 2: bfloat16 [4096, 4096], P(('depth', 'row'), 'col')
- output 3: float32 [4096, 11008], P('row', 'col')
- output 4: float32 [11008, 4096], P('row', 'col')
- output 5: float32 [4096, 4096], P('row', 'col')
- output 6: float32 [4096, 4096], P('row', 'col')
All inputs are finite; a program needn't handle non-finite values.
Results may differ from the reference program's by a relative error of at most 0.001.
Values are sent between devices in bfloat16 or wider.
A program may use at most 1 GiB of HBM per device.

```python
import jax
import jax.numpy as jnp
from jax import lax

TOK_DEV = 1024
D = 4096
FF = 11008
TOKENS = 4096


def setup_inputs(seed: int = 0) -> dict:
    key_list = jax.random.split(jax.random.key(seed), 6)
    tokens = jax.random.normal(key_list[0], (TOKENS, D), jnp.float32)
    w_up = jax.random.normal(key_list[1], (D, FF), jnp.float32) * D ** -0.5
    w_down = jax.random.normal(key_list[2], (FF, D), jnp.float32) * FF ** -0.5
    w_value = jax.random.normal(key_list[3], (D, D), jnp.float32) * D ** -0.5
    w_output = jax.random.normal(key_list[4], (D, D), jnp.float32) * D ** -0.5
    grad_out = jax.random.normal(key_list[5], (TOKENS, D), jnp.float32)
    return {
        "tokens": tokens.astype(jnp.bfloat16),
        "w_up": w_up.astype(jnp.bfloat16),
        "w_down": w_down.astype(jnp.bfloat16),
        "w_value": w_value.astype(jnp.bfloat16),
        "w_output": w_output.astype(jnp.bfloat16),
        "grad_out": grad_out.astype(jnp.bfloat16),
    }


def reference(tokens, w_up, w_down, w_value, w_output, grad_out):
    block_count = TOKENS // TOK_DEV

    def block_step(acc_carry, blk_pair):
        x_blk, g_blk = blk_pair
        pre_act = jnp.dot(x_blk, w_up, preferred_element_type=jnp.float32)
        act_f32, gelu_pull = jax.vjp(jax.nn.gelu, pre_act)
        act_bf16 = act_f32.astype(jnp.bfloat16)
        val_proj = jnp.dot(x_blk, w_value, preferred_element_type=jnp.float32).astype(jnp.bfloat16)
        y_blk = (jnp.dot(act_bf16, w_down, preferred_element_type=jnp.float32)
                 + jnp.dot(val_proj, w_output, preferred_element_type=jnp.float32)).astype(jnp.bfloat16)
        d_act = jnp.dot(g_blk, w_down.T, preferred_element_type=jnp.float32)
        d_pre = gelu_pull(d_act)[0].astype(jnp.bfloat16)
        d_val = jnp.dot(g_blk, w_output.T, preferred_element_type=jnp.float32).astype(jnp.bfloat16)
        dx_blk = (jnp.dot(d_pre, w_up.T, preferred_element_type=jnp.float32)
                  + jnp.dot(d_val, w_value.T, preferred_element_type=jnp.float32)).astype(jnp.bfloat16)
        acc_up, acc_down, acc_value, acc_output = acc_carry
        acc_up = acc_up + jnp.dot(x_blk.T, d_pre, preferred_element_type=jnp.float32)
        acc_down = acc_down + jnp.dot(act_bf16.T, g_blk, preferred_element_type=jnp.float32)
        acc_value = acc_value + jnp.dot(x_blk.T, d_val, preferred_element_type=jnp.float32)
        acc_output = acc_output + jnp.dot(val_proj.T, g_blk, preferred_element_type=jnp.float32)
        return (acc_up, acc_down, acc_value, acc_output), (y_blk, dx_blk)

    grad_init = (
        jnp.zeros((D, FF), jnp.float32),
        jnp.zeros((FF, D), jnp.float32),
        jnp.zeros((D, D), jnp.float32),
        jnp.zeros((D, D), jnp.float32),
    )
    blk_pairs = (tokens.reshape(block_count, TOK_DEV, D), grad_out.reshape(block_count, TOK_DEV, D))
    grad_sums, block_outs = lax.scan(block_step, grad_init, blk_pairs)
    y_out = block_outs[0].reshape(TOKENS, D)
    grad_in = block_outs[1].reshape(TOKENS, D)
    return (y_out, grad_in, grad_sums[0], grad_sums[1], grad_sums[2], grad_sums[3])
```

```python
import jax
import jax.numpy as jnp
from jax import lax
from jax.experimental import pallas as pl
from jax.experimental.pallas import tpu as pltpu
from jax.sharding import PartitionSpec as P


AXES = ("depth", "col", "row")
F32, BF16 = jnp.float32, jnp.bfloat16
NN, NT, TN = ((1,), (0,)), ((1,), (1,)), ((0,), (0,))


def dev(d, c, r):
    return 4 * d + 2 * c + r


GRID = [(d, c, r) for d in (0, 1) for c in (0, 1) for r in (0, 1)]
DIAG = [(d, c, c) for d in (0, 1) for c in (0, 1)]
OFF = [(d, c, 1 - c) for d in (0, 1) for c in (0, 1)]

PX = [(dev(d, c, r), dev(d, 1 - c, r)) for d, c, r in GRID]
PY = [(dev(d, c, r), dev(1 - d, c, r)) for d, c, r in GRID]
PR = [(dev(d, c, r), dev(d, c, 1 - r)) for d, c, r in GRID]
OFF_X = [(dev(d, c, r), dev(d, 1 - c, 1 - r)) for d, c, r in OFF]
OFF_Y = [(dev(d, c, r), dev(1 - d, c, r)) for d, c, r in OFF]
DIAG_TO_OFF = [(dev(d, c, r), dev(d, c, 1 - r)) for d, c, r in DIAG]
OFF_TO_DIAG = [(dev(d, c, r), dev(d, c, 1 - r)) for d, c, r in OFF]
DIAG_X = [(dev(d, c, r), dev(d, 1 - c, r)) for d, c, r in DIAG]
OFF_X_SAME = [(dev(d, c, r), dev(d, 1 - c, r)) for d, c, r in OFF]


def permute(value, pairs):
    return lax.ppermute(value, AXES, pairs)


def product(name, flag, segments, dims, rows, cols, tile_m, tile_n, outs, finish, extra=()):
    lhs_axis, rhs_axis = dims[0][0], dims[1][0]
    operands, specs, plan = [], [], []
    flops = 0

    def add(value, is_lhs, live, column, depth):
        def index(i, j, f):
            place = i if is_lhs else j
            if live is not None:
                place = jnp.where(f[0] == live, place, 0)
            axis = lhs_axis if is_lhs else rhs_axis
            other = 0 if column is None else (f[1] if column == 0 else 1 - f[1])
            return (place, other) if axis == 1 else (other, place)

        tile = tile_m if is_lhs else tile_n
        axis = lhs_axis if is_lhs else rhs_axis
        specs.append(pl.BlockSpec((tile, depth) if axis == 1 else (depth, tile), index))
        operands.append(value)
        return len(operands) - 1

    for lhs, rhs, column in segments:
        first = rhs[0] if isinstance(rhs, tuple) else rhs
        depth = first.shape[rhs_axis]
        flops += 2 * rows * cols * depth
        sides = []
        for value, is_lhs, col in ((lhs, True, column), (rhs, False, None)):
            if isinstance(value, tuple):
                sides.append((add(value[0], is_lhs, 1, col, depth), add(value[1], is_lhs, 0, col, depth)))
            else:
                place = add(value, is_lhs, None, col, depth)
                sides.append((place, place))
        plan.append(sides)
    n_dot = len(operands)
    two_way = any(a[0] != a[1] or b[0] != b[1] for a, b in plan)
    for value in extra:
        specs.append(pl.BlockSpec((tile_m, tile_n), lambda i, j, f: (i, j)))
        operands.append(value)
    n_extra = len(extra)

    def body(flag_ref, *refs):
        extras = refs[n_dot:n_dot + n_extra]
        out_refs = refs[n_dot + n_extra:]

        def run(pick):
            total = None
            for a, b in plan:
                part = lax.dot_general(refs[a[pick]][...], refs[b[pick]][...], (dims, ((), ())),
                                       preferred_element_type=F32)
                total = part if total is None else total + part
            finish(total, extras, out_refs)

        if two_way:
            pl.when(flag_ref[0] == 1)(lambda: run(0))
            pl.when(flag_ref[0] == 0)(lambda: run(1))
        else:
            run(0)

    bytes_accessed = sum(v.size * v.dtype.itemsize for v in operands) + sum(
        rows * cols * jnp.dtype(t).itemsize for t in outs)
    aliases = {1 + n_dot: 0} if name == "dwdn_b" else {}
    result = pl.pallas_call(
        body,
        grid_spec=pltpu.PrefetchScalarGridSpec(
            num_scalar_prefetch=1,
            grid=(pl.cdiv(rows, tile_m), pl.cdiv(cols, tile_n)),
            in_specs=specs,
            out_specs=[pl.BlockSpec((tile_m, tile_n), lambda i, j, f: (i, j))] * len(outs),
        ),
        out_shape=[jax.ShapeDtypeStruct((rows, cols), t) for t in outs],
        input_output_aliases=aliases,
        cost_estimate=pl.CostEstimate(flops=flops, bytes_accessed=bytes_accessed, transcendentals=0),
        compiler_params=pltpu.CompilerParams(vmem_limit_bytes=63000000),
        name=name,
    )(flag, *operands)
    return result[0] if len(outs) == 1 else result


def store(total, extras, outs):
    outs[0][...] = total.astype(outs[0].dtype)


def store_gelu(total, extras, outs):
    outs[0][...] = total
    outs[1][...] = jax.nn.gelu(total).astype(BF16)


def store_gelu_grad(total, extras, outs):
    outs[0][...] = jax.vjp(jax.nn.gelu, extras[0][...])[1](total)[0].astype(BF16)


def store_sum(total, extras, outs):
    outs[0][...] = extras[0][...] + total


def solution(mesh):
    act_spec = P(("depth", "row"), "col")
    wgt_spec = P("row", "col")

    def device_step(x_blk, up_blk, down_blk, val_blk, out_blk, g_blk):
        depth_i, col_i, row_i = (lax.axis_index(a) for a in AXES)
        same = row_i == col_i
        flag = jnp.stack([same.astype(jnp.int32), depth_i.astype(jnp.int32)])
        tok, half = x_blk.shape
        hid = up_blk.shape[1]
        dim = val_blk.shape[1]

        x_far = permute(x_blk, PX)
        up_far = permute(up_blk, PR)
        val_far = permute(val_blk, PR)
        x2 = permute(x_blk, PY)
        x2_far = permute(x_far, PY)
        xr0, xn0 = jnp.where(same, x_blk, x_far), jnp.where(same, x_far, x_blk)
        xr2, xn2 = jnp.where(same, x2, x2_far), jnp.where(same, x2_far, x2)

        quarter = dim // 2
        w_send = lax.dynamic_slice_in_dim(down_blk, depth_i * quarter, quarter, axis=1)
        o_send = lax.dynamic_slice_in_dim(out_blk, depth_i * quarter, quarter, axis=1)
        w_x = permute(w_send, OFF_X)
        o_x = permute(o_send, OFF_X)
        w_y = permute(w_x, OFF_Y)
        o_y = permute(o_x, OFF_Y)
        w_own = permute(down_blk, DIAG_TO_OFF)
        o_own = permute(out_blk, DIAG_TO_OFF)
        w_xd, w_yd = permute(w_x, OFF_TO_DIAG), permute(w_y, OFF_TO_DIAG)
        o_xd, o_yd = permute(o_x, OFF_TO_DIAG), permute(o_y, OFF_TO_DIAG)

        g_far = permute(g_blk, PX)
        g2 = permute(g_blk, PY)
        g2_far = permute(g_far, PY)

        def forward(xr, xn, tag):
            u, a = product("u" + tag, flag, [(xr, up_blk, None), (xn, up_far, None)], NN, tok, hid, 1024, 512,
                           (F32, BF16), store_gelu)
            v = product("v" + tag, flag, [(xr, val_blk, None), (xn, val_far, None)], NN, tok, dim, 1024, 512,
                        (BF16,), store)
            return u, a, v

        u0, a0, v0 = forward(xr0, xn0, "0")
        u2, a2, v2 = forward(xr2, xn2, "2")

        def spread(h0, h2):
            ac = permute(h0, DIAG_X + OFF_TO_DIAG)
            b = permute(h0, OFF_X)
            c = permute(h2, OFF_TO_DIAG)
            yf1 = permute(ac, OFF_Y)
            yf2 = permute(b, OFF_Y)
            return (h0, ac), (ac, b), (h2, yf1), (c, yf2)

        a_blocks = spread(a0, a2)
        v_blocks = spread(v0, v2)

        def backward(gc, gf, u, tag):
            dv = product("dv" + tag, flag, [
                (gc, (out_blk, o_own), None), (gf, (o_xd, o_x), 0), (gf, (o_yd, o_y), 1),
            ], NT, tok, dim, 1024, 512, (BF16,), store)
            du = product("du" + tag, flag, [
                (gc, (down_blk, w_own), None), (gf, (w_xd, w_x), 0), (gf, (w_yd, w_y), 1),
            ], NT, tok, hid, 1024, 512, (BF16,), store_gelu_grad, extra=(u,))
            return du, dv

        du0, dv0 = backward(g_blk, g_far, u0, "0")
        du1, dv1 = permute(du0, PR), permute(dv0, PR)
        e1 = product("dx1", flag, [(du1, up_blk, None), (dv1, val_blk, None)], NT, tok, half, 512, 512, (F32,), store)
        e0 = product("dx0", flag, [(du0, up_blk, None), (dv0, val_blk, None)], NT, tok, half, 512, 512, (F32,), store)
        e_first = permute(jnp.where(same, e1, e0), OFF_X_SAME + DIAG_TO_OFF)
        e_second = permute(e1, OFF_X)
        dx = (jnp.where(same, e0, e_second) + e_first).astype(BF16)

        du2, dv2 = backward(g2, g2_far, u2, "2")
        du3, dv3 = permute(du2, PR), permute(dv2, PR)
        x1, x3 = permute(xn0, PR), permute(xn2, PR)
        xs = (xr0, x1, xr2, x3)
        grad_value = product("dwv", flag, [(x, d, None) for x, d in zip(xs, (dv0, dv1, dv2, dv3))],
                             TN, half, dim, 1024, 512, (F32,), store)
        grad_up = product("dwup", flag, [(x, d, None) for x, d in zip(xs, (du0, du1, du2, du3))],
                          TN, half, hid, 1024, 512, (F32,), store)

        y0 = product("y0", flag, [(a_blocks[0], down_blk, None), (v_blocks[0], out_blk, None)], NN, tok, half, 512, 256,
                     (F32,), store)
        y1 = product("y1", flag, [(a_blocks[1], down_blk, None), (v_blocks[1], out_blk, None)], NN, tok, half, 512, 256,
                     (F32,), store)
        y = (y0 + permute(y1, PR)).astype(BF16)

        g1, g3 = permute(g_blk, PR), permute(g2, PR)

        def down_grad(blocks, width, tag):
            first = product("dwdn_a", flag, [(blocks[0], g_blk, None), (blocks[1], g1, None)], TN, width, half, 1024, 512,
                            (F32,), store)
            return product("dwdn_b", flag, [(blocks[2], g2, None), (blocks[3], g3, None)], TN, width, half, 1024, 512,
                           (F32,), store_sum, extra=(first,))

        grad_output = down_grad(v_blocks, dim, "o")
        grad_down = down_grad(a_blocks, hid, "a")
        return y, dx, grad_up, grad_down, grad_value, grad_output

    return jax.shard_map(
        device_step,
        mesh=mesh,
        in_specs=(act_spec, wgt_spec, wgt_spec, wgt_spec, wgt_spec, act_spec),
        out_specs=(act_spec, act_spec, wgt_spec, wgt_spec, wgt_spec, wgt_spec),
        check_vma=False,
    )
```

```python
import jax
import jax.numpy as jnp
from jax import lax
from jax.experimental import pallas as pl
from jax.experimental.pallas import tpu as pltpu
from jax.sharding import PartitionSpec as P


AXES = ("depth", "col", "row")
F32, BF16 = jnp.float32, jnp.bfloat16
NN, NT, TN = ((1,), (0,)), ((1,), (1,)), ((0,), (0,))


def dev(d, c, r):
    return 4 * d + 2 * c + r


GRID = [(d, c, r) for d in (0, 1) for c in (0, 1) for r in (0, 1)]
DIAG = [(d, c, c) for d in (0, 1) for c in (0, 1)]
OFF = [(d, c, 1 - c) for d in (0, 1) for c in (0, 1)]

PX = [(dev(d, c, r), dev(d, 1 - c, r)) for d, c, r in GRID]
PY = [(dev(d, c, r), dev(1 - d, c, r)) for d, c, r in GRID]
PR = [(dev(d, c, r), dev(d, c, 1 - r)) for d, c, r in GRID]
OFF_X = [(dev(d, c, r), dev(d, 1 - c, 1 - r)) for d, c, r in OFF]
OFF_Y = [(dev(d, c, r), dev(1 - d, c, r)) for d, c, r in OFF]
DIAG_TO_OFF = [(dev(d, c, r), dev(d, c, 1 - r)) for d, c, r in DIAG]
OFF_TO_DIAG = [(dev(d, c, r), dev(d, c, 1 - r)) for d, c, r in OFF]
DIAG_X = [(dev(d, c, r), dev(d, 1 - c, r)) for d, c, r in DIAG]
OFF_X_SAME = [(dev(d, c, r), dev(d, 1 - c, r)) for d, c, r in OFF]


def permute(value, pairs):
    return lax.ppermute(value, AXES, pairs)


def product(flag, segments, dims, rows, cols, tile_m, tile_n, outs, finish, extra=()):
    lhs_axis, rhs_axis = dims[0][0], dims[1][0]
    operands, specs, plan = [], [], []
    flops = 0

    def add(value, is_lhs, live, column, depth):
        def index(i, j, f):
            place = i if is_lhs else j
            if live is not None:
                place = jnp.where(f[0] == live, place, 0)
            axis = lhs_axis if is_lhs else rhs_axis
            other = 0 if column is None else column(f[1])
            return (place, other) if axis == 1 else (other, place)

        tile = tile_m if is_lhs else tile_n
        axis = lhs_axis if is_lhs else rhs_axis
        specs.append(pl.BlockSpec((tile, depth) if axis == 1 else (depth, tile), index))
        operands.append(value)
        return len(operands) - 1

    for lhs, rhs, column in segments:
        first = rhs[0] if isinstance(rhs, tuple) else rhs
        depth = first.shape[rhs_axis]
        flops += 2 * rows * cols * depth
        sides = []
        for value, is_lhs, col in ((lhs, True, column), (rhs, False, None)):
            if isinstance(value, tuple):
                sides.append((add(value[0], is_lhs, 1, col, depth), add(value[1], is_lhs, 0, col, depth)))
            else:
                place = add(value, is_lhs, None, col, depth)
                sides.append((place, place))
        plan.append(sides)
    n_dot = len(operands)
    two_way = any(a[0] != a[1] or b[0] != b[1] for a, b in plan)
    for value in extra:
        specs.append(pl.BlockSpec((tile_m, tile_n), lambda i, j, f: (i, j)))
        operands.append(value)
    n_extra = len(extra)

    def body(flag_ref, *refs):
        extras = refs[n_dot:n_dot + n_extra]
        out_refs = refs[n_dot + n_extra:]

        def run(pick):
            total = None
            for a, b in plan:
                part = lax.dot_general(refs[a[pick]][...], refs[b[pick]][...], (dims, ((), ())),
                                       preferred_element_type=F32)
                total = part if total is None else total + part
            finish(total, extras, out_refs)

        if two_way:
            pl.when(flag_ref[0] == 1)(lambda: run(0))
            pl.when(flag_ref[0] == 0)(lambda: run(1))
        else:
            run(0)

    bytes_accessed = sum(v.size * v.dtype.itemsize for v in operands) + sum(
        rows * cols * jnp.dtype(t).itemsize for t in outs)
    call = pl.pallas_call(
        body,
        grid_spec=pltpu.PrefetchScalarGridSpec(
            num_scalar_prefetch=1,
            grid=(pl.cdiv(rows, tile_m), pl.cdiv(cols, tile_n)),
            in_specs=specs,
            out_specs=[pl.BlockSpec((tile_m, tile_n), lambda i, j, f: (i, j))] * len(outs),
        ),
        out_shape=[jax.ShapeDtypeStruct((rows, cols), t) for t in outs],
        cost_estimate=pl.CostEstimate(flops=flops, bytes_accessed=bytes_accessed, transcendentals=0),
        compiler_params=pltpu.CompilerParams(vmem_limit_bytes=63000000),
    )
    result = call(flag, *operands)
    return result[0] if len(outs) == 1 else result


def store(total, extras, outs):
    outs[0][...] = total.astype(outs[0].dtype)


def store_gelu(total, extras, outs):
    scale, cubic = 0.7978845608028654, 0.044715
    square = total * total
    tanh = jnp.tanh(scale * (total + cubic * (total * square)))
    cdf = 0.5 * (1.0 + tanh)
    outs[0][...] = cdf + (0.5 * scale) * total * (1.0 - tanh * tanh) * (1.0 + (3.0 * cubic) * square)
    outs[1][...] = (total * cdf).astype(BF16)


def store_with(total, extras, outs):
    outs[0][...] = (total + extras[0][...]).astype(outs[0].dtype)


def store_times(total, extras, outs):
    outs[0][...] = (total * extras[0][...]).astype(outs[0].dtype)


def store_with_times(total, extras, outs):
    outs[0][...] = ((total + extras[1][...]) * extras[0][...]).astype(outs[0].dtype)


def solution(mesh):
    act_spec = P(("depth", "row"), "col")
    wgt_spec = P("row", "col")

    def device_step(x_blk, up_blk, down_blk, val_blk, out_blk, g_blk):
        depth_i, col_i, row_i = (lax.axis_index(a) for a in AXES)
        same = row_i == col_i
        flag = jnp.stack([same.astype(jnp.int32), depth_i.astype(jnp.int32)])
        tok, half = x_blk.shape
        hid = up_blk.shape[1]
        dim = val_blk.shape[1]

        x_far = permute(x_blk, PX)
        x2 = permute(x_blk, PY)
        x2_far = permute(x_far, PY)
        o_own, w_own = permute(out_blk, PR), permute(down_blk, PR)
        val_far, up_far = permute(val_blk, PR), permute(up_blk, PR)
        xr0, xn0 = jnp.where(same, x_blk, x_far), jnp.where(same, x_far, x_blk)
        xr2, xn2 = jnp.where(same, x2, x2_far), jnp.where(same, x2_far, x2)
        x1, x3 = permute(xn0, PR), permute(xn2, PR)

        part = dim // 4
        o_x = permute(lax.dynamic_slice_in_dim(out_blk, depth_i * 2 * part, 2 * part, axis=1), OFF_X)
        o_y, o_xd = permute(o_x, OFF_Y), permute(o_x, PR)
        o_yd = permute(o_y, PR)
        far_w = []
        for k in (0, 1):
            sent = lax.dynamic_slice_in_dim(down_blk, (depth_i * 2 + k) * part, part, axis=1)
            w_x = permute(sent, OFF_X)
            w_y, w_xd = permute(w_x, OFF_Y), permute(w_x, PR)
            w_yd = permute(w_y, PR)
            far_w.append(((w_xd, w_x), lambda d, k=k: 2 * d + k))
            far_w.append(((w_yd, w_y), lambda d, k=k: 2 * (1 - d) + k))

        g_far = permute(g_blk, PX)
        g2 = permute(g_blk, PY)
        g2_far = permute(g_far, PY)
        g1, g3 = permute(g_blk, PR), permute(g2, PR)

        def forward(xr, xn):
            v = product(flag, [(xr, val_blk, None), (xn, val_far, None)], NN, tok, dim, 1024, 512,
                        (BF16,), store)
            slope, a = product(flag, [(xr, up_blk, None), (xn, up_far, None)], NN, tok, hid, 1024, 512,
                           (F32, BF16), store_gelu)
            return slope, a, v

        slope0, a0, v0 = forward(xr0, xn0)
        slope2, a2, v2 = forward(xr2, xn2)

        def spread(h0, h2):
            ac = permute(h0, DIAG_X + OFF_TO_DIAG)
            b = permute(h0, OFF_X)
            c = permute(h2, PR)
            yf1 = permute(ac, OFF_Y)
            yf2 = permute(b, OFF_Y)
            return (h0, ac), (ac, b), (h2, yf1), (c, yf2)

        v_blocks = spread(v0, v2)
        a_blocks = spread(a0, a2)

        near_v = (g_blk, (out_blk, o_own), None)
        near_u = (g_blk, (down_blk, w_own), None)
        pdv0 = product(flag, [near_v], NT, tok, dim, 1024, 512, (F32,), store)
        pdu0 = product(flag, [near_u], NT, tok, hid, 1024, 512, (F32,), store)

        def far(g):
            far_v = [(g, (o_xd, o_x), lambda d: d), (g, (o_yd, o_y), lambda d: 1 - d)]
            return far_v, [(g, w, column) for w, column in far_w]

        far_v, far_u = far(g_far)
        dv0 = product(flag, far_v, NT, tok, dim, 1024, 512, (BF16,), store_with, extra=(pdv0,))
        du0 = product(flag, far_u, NT, tok, hid, 1024, 512, (BF16,), store_with_times, extra=(slope0, pdu0))
        dv1, du1 = permute(dv0, PR), permute(du0, PR)
        e0 = product(flag, [(du0, up_blk, None), (dv0, val_blk, None)], NT, tok, half, 512, 512, (F32,), store)
        e1 = product(flag, [(du1, up_blk, None), (dv1, val_blk, None)], NT, tok, half, 512, 512, (F32,), store)
        e_second = permute(e1, OFF_X)
        e_first = permute(jnp.where(same, e1, e0), OFF_X_SAME + DIAG_TO_OFF)
        dx = (jnp.where(same, e0, e_second) + e_first).astype(BF16)

        far_v, far_u = far(g2_far)
        dv2 = product(flag, [(g2,) + near_v[1:]] + far_v, NT, tok, dim, 1024, 512, (BF16,), store)
        du2 = product(flag, [(g2,) + near_u[1:]] + far_u, NT, tok, hid, 1024, 512, (BF16,), store_times,
                      extra=(slope2,))
        dv3, du3 = permute(dv2, PR), permute(du2, PR)

        def part_y(block):
            return product(flag, [(a_blocks[block], down_blk, None), (v_blocks[block], out_blk, None)], NN,
                           tok, half, 512, 512, (F32,), store)

        y0, y1 = part_y(0), part_y(1)
        y = (y0 + permute(y1, PR)).astype(BF16)

        xs, gs = (xr0, x1, xr2, x3), (g_blk, g1, g2, g3)

        def gradient(left, right, rows, cols, tile_m, tile_n):
            segments = [(a, b, None) for a, b in zip(left, right)]
            return product(flag, segments, TN, rows, cols, tile_m, tile_n, (F32,), store)

        grad_value = gradient(xs, (dv0, dv1, dv2, dv3), half, dim, 1024, 512)
        grad_up = gradient(xs, (du0, du1, du2, du3), half, hid, 1024, 512)
        grad_output = gradient(v_blocks, gs, dim, half, 256, 2048)
        grad_down = gradient(a_blocks, gs, hid, half, 256, 2048)
        return y, dx, grad_up, grad_down, grad_value, grad_output

    return jax.shard_map(
        device_step,
        mesh=mesh,
        in_specs=(act_spec, wgt_spec, wgt_spec, wgt_spec, wgt_spec, act_spec),
        out_specs=(act_spec, act_spec, wgt_spec, wgt_spec, wgt_spec, wgt_spec),
        check_vma=False,
    )
```
